32 devices in a mesh: tile: 16 (over z, x, core), mem: 2 (over y).
Axes of the slice: x: 2, y: 2, z: 4, core: 2. Of those that a mesh axis runs over, the one named last changes fastest.
Arguments:
- anomalies: bfloat16 [80, 137, 2048], P('mem', None, 'tile'), may hold values from -6 to 6
- analysis_weights: bfloat16 [16, 80, 80], P('tile'), may hold values from -0.6 to 1.7
- background_mean: bfloat16 [137, 2048], P(None, 'tile'), may hold values from -6 to 6
- background: bfloat16 [80, 137, 2048], P('mem', None, 'tile'), may hold values from -6 to 6
- jacobian_table: bfloat16 [8461, 137], replicated, may hold values from -0.5 to 0.5
- channel_list: int32 [96], replicated, may hold values from 0 to 8460
- send_slots: int32 [16, 16, 32], P('tile'), may hold values from -1 to 127, as said below
- footprint: int32 [8192, 4], P('tile'), may hold values from 0 to 511, as said below
- footprint_weight: bfloat16 [8192, 4], P('tile'), may hold values from 0.25 to 1
- channel_bias: float32 [96], replicated, may hold values from -4 to 4
Outputs:
- analysis_members: bfloat16 [80, 137, 2048], P('mem', None, 'tile')
- radiance_prior: float32 [96, 80, 8192], P(None, 'mem', 'tile')
The draws below stay inside these ranges and needn't reach their ends.
Inputs may be any that keep to these rules, and one draw needn't show every extreme that they name: `send_slots`: entry [s, d, i] is a column within owner s's block of 128 columns that owner s sends to tile d in slot i, or -1 for an empty slot; the filled slots of a pair come first, each pair fills 1 to 32 slots, and in every draw one tile receives 32 filled slots from every owner. `footprint`: entry [o, j] is a slot of the buffer of observation o's tile, which holds 32 slots from each owner in owner order; every entry names a filled slot, the 4 entries of a row differ, and every filled slot is named by some row of that tile.
All inputs are finite; a program needn't handle non-finite values.
Results may differ from the reference program's by a relative error of at most 0.0021.
Values may be sent and summed in bfloat16 or wider, within the bound.
A program may use at most 128 MiB of HBM per device.

```python
import math
import jax
import jax.numpy as jnp
from jax import lax

MEMBERS = 80
LEVELS = 137
SPECTRUM = 8461
CHANNELS = 96
COLS_DEV = 128
GROUP = 128
SLOTS = 32
OBS_DEV = 512
FOOT = 4
COLUMNS = 2048
POINTS = 16
OBSERVATIONS = 8192
N_TILE = 16


def draw_analysis_weights(key, part):
    identity = jnp.eye(MEMBERS, dtype=jnp.float32)[None]
    noise_draw = jnp.clip(jax.random.normal(jax.random.fold_in(key, 1), (POINTS, MEMBERS, MEMBERS), jnp.float32), -4.0, 4.0)
    diag_part = identity
    return (diag_part + noise_draw * (0.6 / math.sqrt(MEMBERS))).astype(jnp.bfloat16)


def slot_counts(key):
    tile_count = COLUMNS // COLS_DEV
    uniform_part = jax.random.randint(jax.random.fold_in(key, 11), (tile_count, tile_count), 1, SLOTS + 1)
    receiver_load = jax.random.randint(jax.random.fold_in(key, 12), (1, tile_count), 1, 5)
    counts = jnp.clip(uniform_part * receiver_load // 3, 1, SLOTS)
    full_receiver = jax.random.randint(jax.random.fold_in(key, 13), (), 0, tile_count)
    counts = jnp.where(jnp.arange(tile_count)[None, :] == full_receiver, SLOTS, counts)
    return counts.astype(jnp.int32)


def draw_send_slots(key, part):
    tile_count = COLUMNS // COLS_DEV
    counts = slot_counts(key)
    columns = jax.random.randint(jax.random.fold_in(key, 14), (tile_count, tile_count, SLOTS), 0, COLS_DEV)
    filled = jnp.arange(SLOTS)[None, None, :] < counts[:, :, None]
    return jnp.where(filled, columns, -1).astype(jnp.int32)


def draw_footprint(key, part):
    tile_count = COLUMNS // COLS_DEV
    buffer_size = tile_count * SLOTS
    counts = slot_counts(key)
    filled = jnp.arange(SLOTS)[None, None, :] < jnp.transpose(counts)[:, :, None]
    filled = filled.reshape(tile_count, buffer_size)
    receiver_keys = jax.random.split(jax.random.fold_in(key, 15), tile_count)

    def shuffle_one(subkey):
        return jax.random.permutation(subkey, buffer_size).astype(jnp.int32)
    shuffle = jax.vmap(shuffle_one)(receiver_keys)
    scores = jnp.where(filled, shuffle, buffer_size + shuffle)
    slot_order = jnp.argsort(scores, axis=1, stable=True).astype(jnp.int32)
    filled_count = jnp.sum(filled.astype(jnp.int32), axis=1, keepdims=True)
    position = jnp.arange(OBS_DEV * FOOT, dtype=jnp.int32)[None, :] % filled_count
    foot_slots = jnp.take_along_axis(slot_order, position, axis=1)
    return foot_slots.reshape(tile_count * OBS_DEV, FOOT).astype(jnp.int32)


def set_ends(entries, stream_key, low, high):
    longest = entries.shape.index(max(entries.shape))
    spots = []
    for shift in (0, 1):
        where = [jax.random.randint(jax.random.fold_in(stream_key, axis), (), 0, length) for axis, length in enumerate(entries.shape)]
        where[longest] = (where[longest] + shift) % entries.shape[longest]
        spots.append(tuple(where))
    return entries.at[spots[0]].set(low).at[spots[1]].set(high)


def levels(key, extent, shards, low, largest):
    factor_of = 1.0
    for dim, parts in shards:
        draws = jax.random.uniform(jax.random.fold_in(jax.random.fold_in(key, 6), dim), (parts,), jnp.float32, low / len(shards), largest / len(shards))
        factor_of = factor_of * jnp.repeat(jnp.exp(draws), extent[dim] // parts).reshape((-1,) + (1,) * (len(extent) - 1 - dim))
    return factor_of


def gaussian(rng, shape, scale, limit, shards=(), kind=jnp.bfloat16):
    values = scale * jax.random.normal(rng, shape, jnp.float32)
    if shards:
        values = values * levels(rng, shape, shards, -0.22, 0.18)
    return jnp.clip(values, -limit, limit).astype(kind)


def setup_inputs(seed: int = 0) -> dict:
    key_list = jax.random.split(jax.random.key(seed), 11)
    anomalies = gaussian(key_list[0], (MEMBERS, LEVELS, COLUMNS), 1.0, 6.0, ((0, 2), (2, 16)))
    analysis_weights = draw_analysis_weights(jax.random.fold_in(key_list[10], 71), 0)
    background_mean = gaussian(key_list[2], (LEVELS, COLUMNS), 1.0, 6.0, ((1, 16),))
    background = gaussian(key_list[3], (MEMBERS, LEVELS, COLUMNS), 1.0, 6.0, ((0, 2), (2, 16)))
    jacobian_table = gaussian(key_list[4], (SPECTRUM, LEVELS), LEVELS ** -0.5, 0.5)
    channel_list = set_ends(jax.random.randint(key_list[5], (CHANNELS,), 0, SPECTRUM), jax.random.fold_in(key_list[5], 1), 0, SPECTRUM - 1).astype(jnp.int32)
    send_slots = draw_send_slots(jax.random.fold_in(key_list[10], 71), 0)
    footprint = draw_footprint(jax.random.fold_in(key_list[10], 71), 0)
    footprint_weight = jnp.clip(jnp.exp(math.log(1.0) - 1.3862944 * jax.random.uniform(key_list[8], (OBSERVATIONS, FOOT), jnp.float32) ** levels(key_list[8], (OBSERVATIONS, FOOT), ((0, 16),), -0.2, 0.2)), 0.25, 1.0).astype(jnp.bfloat16)
    channel_bias = gaussian(key_list[9], (CHANNELS,), 1.0, 4.0, (), jnp.float32)
    return {"anomalies": anomalies, "analysis_weights": analysis_weights, "background_mean": background_mean, "background": background, "jacobian_table": jacobian_table, "channel_list": channel_list, "send_slots": send_slots, "footprint": footprint, "footprint_weight": footprint_weight, "channel_bias": channel_bias}


def reference(anomalies, analysis_weights, background_mean, background, jacobian_table, channel_list, send_slots, footprint, footprint_weight, channel_bias):
    points = analysis_weights.shape[0]
    shaped = anomalies.astype(jnp.float32).reshape(MEMBERS, LEVELS, points, GROUP)
    mixture = jnp.einsum('klgc,gkm->mlgc', shaped, analysis_weights.astype(jnp.float32))
    mixture = mixture.reshape(MEMBERS, LEVELS, points * GROUP)
    analysis_members = (background_mean.astype(jnp.float32)[None] + mixture).astype(jnp.bfloat16)

    selected = jnp.take(jacobian_table, channel_list, axis=0).astype(jnp.float32)
    foot_slots = footprint.reshape(N_TILE, OBS_DEV, FOOT)
    foot_weight = footprint_weight.astype(jnp.float32).reshape(N_TILE, OBS_DEV, FOOT)

    def per_receiver(receiver):
        slot_ids = lax.dynamic_index_in_dim(foot_slots, receiver, 0, keepdims=False)
        weight = lax.dynamic_index_in_dim(foot_weight, receiver, 0, keepdims=False)
        source = (slot_ids // SLOTS).astype(jnp.int32)
        slot_place = (slot_ids % SLOTS).astype(jnp.int32)
        local_col = send_slots[source, receiver, slot_place]
        column = (source * COLS_DEV + local_col).astype(jnp.int32)
        profiles = jnp.take(background, column.reshape(-1), axis=2).astype(jnp.float32)
        radiance = jnp.einsum('cl,kls->cks', selected, profiles).astype(jnp.bfloat16)
        radiance = lax.optimization_barrier(radiance).astype(jnp.float32)
        radiance = radiance.reshape(CHANNELS, MEMBERS, OBS_DEV, FOOT)
        combined = jnp.sum(radiance * weight[None, None], axis=3)
        return combined + channel_bias.astype(jnp.float32)[:, None, None]

    stacked = lax.map(per_receiver, jnp.arange(N_TILE, dtype=jnp.int32))
    radiance_prior = jnp.transpose(stacked, (1, 2, 0, 3)).reshape(CHANNELS, MEMBERS, N_TILE * OBS_DEV)
    return analysis_members, radiance_prior
```

```python
import functools

import jax
import jax.numpy as jnp
from jax import lax
from jax.experimental import pallas as pl
from jax.experimental.pallas import tpu as pltpu
from jax.sharding import PartitionSpec as P

LANES = 128
MESH = pl.DeviceIdType.MESH


def exchange_kernel(
    n,
    nm,
    owned_ref,
    target_ref,
    anom_ref,
    weight_ref,
    mean_ref,
    foot_ref,
    fweight_ref,
    recv_ref,
    analysis_ref,
    spread_ref,
    send_buf,
    pieces,
    mixed,
    spread,
    a_send,
    a_recv,
    m_send,
    m_recv,
    local_sem,
):
    tile = lax.axis_index("tile")
    mem = lax.axis_index("mem")
    groups, rows, cols = owned_ref.shape
    chips = n // 2
    slots = spread_ref.shape[0] // n
    obs = spread_ref.shape[1]
    levels = anom_ref.shape[0]

    barrier = pltpu.get_barrier_semaphore()

    def greet(k, carry):
        pl.semaphore_signal(
            barrier, inc=1, device_id=(lax.rem(tile + k, n), mem), device_id_type=MESH
        )
        return carry

    lax.fori_loop(1, n, greet, 0)
    for k in range(1, nm):
        pl.semaphore_signal(
            barrier, inc=1, device_id=(tile, lax.rem(mem + k, nm)), device_id_type=MESH
        )
    own_piece = pltpu.make_async_copy(anom_ref, pieces.at[mem], local_sem.at[0])
    own_piece.start()
    pl.semaphore_wait(barrier, n - 1 + nm - 1)

    def member_copy(k):
        peer = lax.rem(mem + k, nm)
        return pltpu.make_async_remote_copy(
            src_ref=anom_ref,
            dst_ref=pieces.at[mem],
            send_sem=m_send.at[k],
            recv_sem=m_recv.at[k],
            device_id=(tile, peer),
            device_id_type=MESH,
        )

    for k in range(1, nm):
        member_copy(k).start()

    def tile_copy(dest):
        return pltpu.make_async_remote_copy(
            src_ref=send_buf.at[dest],
            dst_ref=recv_ref.at[tile],
            send_sem=a_send.at[dest],
            recv_sem=a_recv.at[tile],
            device_id=(dest, mem),
            device_id_type=MESH,
        )

    def arrival(source):
        return pltpu.make_async_remote_copy(
            src_ref=send_buf.at[source],
            dst_ref=recv_ref.at[source],
            send_sem=a_send.at[source],
            recv_sem=a_recv.at[source],
            device_id=(source, mem),
            device_id_type=MESH,
        )

    my_chip = tile // 2

    def chip_at(p):
        step = ((p + 1) // 2) * (1 - 2 * lax.rem(p + 1, 2))
        return lax.rem(my_chip + step + chips, chips)

    wide = jnp.concatenate([owned_ref[g] for g in range(groups)], axis=1)
    row_id = lax.broadcasted_iota(jnp.int32, (groups * cols, 2 * LANES), 0)

    def pack(chip):
        first = chip * 2
        want = jnp.concatenate([target_ref[first], target_ref[first + 1]], axis=1)
        pick = jnp.where(row_id == want, 1.0, 0.0).astype(jnp.bfloat16)
        out = jnp.dot(wide, pick, preferred_element_type=jnp.float32).astype(jnp.bfloat16)
        send_buf[first] = out[:, :LANES]
        send_buf[first + 1] = out[:, LANES:]

    def send(chip):
        for core in range(2):
            tile_copy(chip * 2 + core).start()

    pack(chip_at(1))

    def step(p, carry):
        pack(chip_at(p))
        send(chip_at(p - 1))
        return carry

    lax.fori_loop(2, chips, step, 0)
    pack(my_chip)
    send(chip_at(chips - 1))
    other = my_chip * 2 + 1 - lax.rem(tile, 2)

    fweight = fweight_ref[...].astype(jnp.float32)

    def spread_rows(s, carry):
        ids = lax.broadcasted_iota(jnp.int32, (slots, obs), 0) + s * slots
        total = jnp.zeros((slots, obs), jnp.float32)
        for j in range(foot_ref.shape[0]):
            total = total + jnp.where(
                ids == foot_ref[j : j + 1, :], fweight[j : j + 1, :], 0.0
            )
        spread[pl.ds(pl.multiple_of(s * slots, slots), slots), :] = total.astype(jnp.bfloat16)
        return carry

    lax.fori_loop(0, n, spread_rows, 0)
    tile_copy(other).start()
    own_chunk = pltpu.make_async_copy(send_buf.at[tile], recv_ref.at[tile], local_sem.at[1])
    own_chunk.start()

    own_piece.wait()
    spread_out = pltpu.make_async_copy(spread, spread_ref, local_sem.at[2])
    spread_out.start()
    for k in range(1, nm):
        member_copy(k).wait()

    def mix(l, carry):
        total = jnp.broadcast_to(
            mean_ref[l].astype(jnp.float32), (weight_ref.shape[1], cols)
        )
        mixture = jnp.zeros_like(total)
        for p in range(nm):
            mixture = mixture + jnp.dot(
                weight_ref[p], pieces[p, l], preferred_element_type=jnp.float32
            )
        mixed[l] = (total + mixture).astype(jnp.bfloat16)
        return carry

    lax.fori_loop(0, levels, mix, 0)

    def drain(k, carry):
        source = lax.rem(tile + k, n)
        arrival(source).wait()
        return carry

    lax.fori_loop(1, n // 2, drain, 0)
    analysis_out = pltpu.make_async_copy(mixed, analysis_ref, local_sem.at[3])
    analysis_out.start()
    lax.fori_loop(n // 2, n, drain, 0)
    own_chunk.wait()
    spread_out.wait()
    analysis_out.wait()


def combine_kernel(n, groups, per_step, bias_ref, recv_ref, spread_ref, out_ref):
    step = pl.program_id(0)
    slots = spread_ref.shape[0] // n
    per_group = out_ref.shape[1] * pl.num_programs(0)
    members = out_ref.shape[2]
    blocks = [recv_ref[s] for s in range(n)]
    for g in range(groups):
        lanes = slice(g * slots, (g + 1) * slots)
        stacked = jnp.concatenate([block[:, lanes] for block in blocks], axis=1)
        prior = jnp.dot(stacked, spread_ref[...], preferred_element_type=jnp.float32)
        for c in range(per_step):
            bias = bias_ref[g * per_group + step * per_step + c]
            out_ref[g, c] = prior[c * members : (c + 1) * members, :] + bias


def shards(
    n,
    nm,
    anomalies,
    analysis_weights,
    background_mean,
    background,
    jacobian_table,
    channel_list,
    send_slots,
    footprint,
    footprint_weight,
    channel_bias,
):
    mem_dev, levels, cols = anomalies.shape
    channels = channel_list.shape[0]
    slots = send_slots.shape[2]
    obs = footprint.shape[0]
    groups = LANES // slots
    rows = channels * mem_dev // groups
    mem = lax.axis_index("mem")

    chosen = (
        jnp.arange(jacobian_table.shape[0], dtype=jnp.int32)[:, None] == channel_list[None, :]
    ).astype(jnp.bfloat16)
    selected = jnp.einsum(
        "sl,sc->cl", jacobian_table, chosen, preferred_element_type=jnp.float32
    ).astype(jnp.bfloat16)
    owned = jnp.einsum(
        "cl,klx->ckx", selected, background, preferred_element_type=jnp.float32
    ).astype(jnp.bfloat16)
    owned = owned.reshape(groups, rows, cols)
    lane_rows = jnp.maximum(send_slots[0], 0)[:, None, :] + (
        jnp.arange(groups, dtype=jnp.int32) * cols
    )[None, :, None]
    target = lane_rows.reshape(n, 1, LANES)
    weights = lax.dynamic_slice_in_dim(analysis_weights[0], mem * mem_dev, mem_dev, 1)
    weights = jnp.transpose(weights.reshape(nm, mem_dev, mem_dev), (0, 2, 1))
    vmem = pl.BlockSpec(memory_space=pltpu.VMEM)
    hbm = pl.BlockSpec(memory_space=pl.ANY)
    received, analysis, spread = pl.pallas_call(
        functools.partial(exchange_kernel, n, nm),
        out_shape=(
            jax.ShapeDtypeStruct((n, rows, LANES), jnp.bfloat16),
            jax.ShapeDtypeStruct((levels, mem_dev, cols), jnp.bfloat16),
            jax.ShapeDtypeStruct((n * slots, obs), jnp.bfloat16),
        ),
        in_specs=[vmem, vmem, hbm, vmem, vmem, vmem, vmem],
        out_specs=(hbm, hbm, hbm),
        scratch_shapes=[
            pltpu.VMEM((n, rows, LANES), jnp.bfloat16),
            pltpu.VMEM((nm, levels, mem_dev, cols), jnp.bfloat16),
            pltpu.VMEM((levels, mem_dev, cols), jnp.bfloat16),
            pltpu.VMEM((n * slots, obs), jnp.bfloat16),
            pltpu.SemaphoreType.DMA((n,)),
            pltpu.SemaphoreType.DMA((n,)),
            pltpu.SemaphoreType.DMA((nm,)),
            pltpu.SemaphoreType.DMA((nm,)),
            pltpu.SemaphoreType.DMA((4,)),
        ],
        compiler_params=pltpu.CompilerParams(
            collective_id=0, has_side_effects=True, vmem_limit_bytes=48 * 1024 * 1024
        ),
        name="exchange",
    )(
        owned,
        target,
        jnp.transpose(anomalies, (1, 0, 2)),
        weights,
        background_mean[:, None, :],
        jnp.transpose(footprint),
        jnp.transpose(footprint_weight),
    )
    analysis_members = jnp.transpose(analysis, (1, 0, 2))

    per_group = channels // groups
    per_step = next(c for c in (4, 8, per_group) if c * mem_dev % 16 == 0)
    prior = pl.pallas_call(
        functools.partial(combine_kernel, n, groups, per_step),
        out_shape=jax.ShapeDtypeStruct((groups, per_group, mem_dev, obs), jnp.float32),
        grid=(per_group // per_step,),
        in_specs=[
            pl.BlockSpec(memory_space=pltpu.SMEM),
            pl.BlockSpec((n, per_step * mem_dev, LANES), lambda i: (0, i, 0)),
            pl.BlockSpec((n * slots, obs), lambda i: (0, 0)),
        ],
        out_specs=pl.BlockSpec((groups, per_step, mem_dev, obs), lambda i: (0, i, 0, 0)),
        compiler_params=pltpu.CompilerParams(vmem_limit_bytes=48 * 1024 * 1024),
        name="combine",
    )(channel_bias, received, spread)
    return analysis_members, prior.reshape(channels, mem_dev, obs)


def solution(mesh):
    placed = (
        P("mem", None, "tile"),
        P("tile", None, None),
        P(None, "tile"),
        P("mem", None, "tile"),
        P(),
        P(),
        P("tile", None, None),
        P("tile", None),
        P("tile", None),
        P(),
    )
    return jax.shard_map(
        functools.partial(shards, mesh.shape["tile"], mesh.shape["mem"]),
        mesh=mesh,
        in_specs=placed,
        out_specs=(P("mem", None, "tile"), P(None, "mem", "tile")),
        check_vma=False,
    )
```

```python
import functools

import jax
import jax.numpy as jnp
from jax import lax
from jax.experimental import pallas as pl
from jax.experimental.pallas import tpu as pltpu
from jax.sharding import PartitionSpec as P

LANES = 128
MESH = pl.DeviceIdType.MESH


def exchange_kernel(
    n,
    nm,
    owned_ref,
    target_ref,
    anom_ref,
    weight_ref,
    mean_ref,
    foot_ref,
    fweight_ref,
    recv_ref,
    analysis_ref,
    spread_ref,
    send_buf,
    relay_buf,
    relay_block,
    relay_target,
    pieces,
    mixed,
    spread,
    a_send,
    a_recv,
    m_send,
    m_recv,
    b_send,
    b_recv,
    r_send,
    local_sem,
):
    tile = lax.axis_index("tile")
    mem = lax.axis_index("mem")
    groups, rows, cols = owned_ref.shape
    chips = n // 2
    slots = spread_ref.shape[0] // n
    obs = spread_ref.shape[1]
    levels = anom_ref.shape[0]

    barrier = pltpu.get_barrier_semaphore()

    def greet(k, carry):
        pl.semaphore_signal(
            barrier, inc=1, device_id=(lax.rem(tile + k, n), mem), device_id_type=MESH
        )
        return carry

    lax.fori_loop(1, n, greet, 0)
    for k in range(1, nm):
        pl.semaphore_signal(
            barrier, inc=1, device_id=(tile, lax.rem(mem + k, nm)), device_id_type=MESH
        )
    own_piece = pltpu.make_async_copy(anom_ref, pieces.at[mem], local_sem.at[0])
    own_piece.start()
    pl.semaphore_wait(barrier, n - 1 + nm - 1)

    def member_copy(k):
        peer = lax.rem(mem + k, nm)
        return pltpu.make_async_remote_copy(
            src_ref=anom_ref,
            dst_ref=pieces.at[mem],
            send_sem=m_send.at[k],
            recv_sem=m_recv.at[k],
            device_id=(tile, peer),
            device_id_type=MESH,
        )

    for k in range(1, nm):
        member_copy(k).start()

    zone_tiles = n // 4
    zone_chips = chips // 4
    zone = tile // zone_tiles
    far_half = zone // 2
    near = zone - 3 * far_half
    depth = near * (1 - 2 * far_half)
    inner = depth == 1
    partner = lax.rem(tile + (1 - 2 * far_half) * zone_tiles + n, n)
    my_chip = tile // 2
    my_place = lax.rem(my_chip, zone_chips)
    halves = relay_split(rows)
    part = rows // halves

    def block_copies():
        for h in range(halves):
            span = (slice(None), pl.ds(h * part, part), slice(None))
            yield pltpu.make_async_remote_copy(
                src_ref=owned_ref.at[span],
                dst_ref=relay_block.at[span],
                send_sem=b_send.at[h],
                recv_sem=b_recv.at[h],
                device_id=(partner, mem),
                device_id_type=MESH,
            )
        yield pltpu.make_async_remote_copy(
            src_ref=target_ref,
            dst_ref=relay_target,
            send_sem=b_send.at[halves],
            recv_sem=b_recv.at[halves],
            device_id=(partner, mem),
            device_id_type=MESH,
        )

    @pl.when(inner)
    def _():
        for copy in reversed(list(block_copies())):
            copy.start()

    def tile_copy(dest):
        return pltpu.make_async_remote_copy(
            src_ref=send_buf.at[dest],
            dst_ref=recv_ref.at[tile],
            send_sem=a_send.at[dest],
            recv_sem=a_recv.at[tile],
            device_id=(dest, mem),
            device_id_type=MESH,
        )

    def relay_copy(h, dest):
        return pltpu.make_async_remote_copy(
            src_ref=relay_buf.at[dest, pl.ds(h * part, part)],
            dst_ref=recv_ref.at[partner, pl.ds(h * part, part)],
            send_sem=r_send.at[h, dest],
            recv_sem=a_recv.at[partner],
            device_id=(dest, mem),
            device_id_type=MESH,
        )

    def arrival(source):
        return pltpu.make_async_remote_copy(
            src_ref=send_buf.at[source],
            dst_ref=recv_ref.at[source],
            send_sem=a_send.at[source],
            recv_sem=a_recv.at[source],
            device_id=(source, mem),
            device_id_type=MESH,
        )

    def chip_of(their_zone, r):
        their_zone = their_zone + far_half * (3 - 2 * their_zone)
        return their_zone * zone_chips + lax.rem(my_place + r, zone_chips)

    def direct_chip(j):
        k = j // zone_chips
        outer_zone = k + (k // 2) * (5 - 2 * k)
        return chip_of(outer_zone + depth * (1 - k - outer_zone), lax.rem(j, zone_chips))

    row_id = lax.broadcasted_iota(jnp.int32, (groups * cols, 2 * LANES), 0)

    def pack(wide, table_ref, chip, out_ref, span):
        first = chip * 2
        want = jnp.concatenate([table_ref[first], table_ref[first + 1]], axis=1)
        pick = jnp.where(row_id == want, 1.0, 0.0).astype(jnp.bfloat16)
        out = jnp.dot(wide, pick, preferred_element_type=jnp.float32).astype(jnp.bfloat16)
        out_ref[first, span] = out[:, :LANES]
        out_ref[first + 1, span] = out[:, LANES:]

    def send(chip):
        for core in range(2):
            dest = chip * 2 + core

            @pl.when(dest != tile)
            def _():
                tile_copy(dest).start()

    wide = jnp.concatenate([owned_ref[g] for g in range(groups)], axis=1)
    whole = slice(None)
    pack(wide, target_ref, direct_chip(0), send_buf, whole)

    def step(j, carry):
        pack(wide, target_ref, direct_chip(j), send_buf, whole)
        send(direct_chip(j - 1))
        return carry

    steps = zone_chips * (4 - 2 * depth)
    lax.fori_loop(1, steps, step, 0)
    own_chunk = pltpu.make_async_copy(send_buf.at[tile], recv_ref.at[tile], local_sem.at[1])
    own_chunk.start()

    fweight = fweight_ref[...].astype(jnp.float32)

    def spread_rows(s, carry):
        ids = lax.broadcasted_iota(jnp.int32, (slots, obs), 0) + s * slots
        total = jnp.zeros((slots, obs), jnp.float32)
        for j in range(foot_ref.shape[0]):
            total = total + jnp.where(
                ids == foot_ref[j : j + 1, :], fweight[j : j + 1, :], 0.0
            )
        spread[pl.ds(pl.multiple_of(s * slots, slots), slots), :] = total.astype(jnp.bfloat16)
        return carry

    lax.fori_loop(0, n // 2, spread_rows, 0)
    send(direct_chip(steps - 1))

    def relay_chip(j):
        return chip_of(j // zone_chips, lax.rem(j, zone_chips))

    relay_own = pltpu.make_async_copy(relay_buf.at[tile], recv_ref.at[partner], local_sem.at[4])

    def relay_send(h, j):
        for core in range(2):
            dest = relay_chip(j) * 2 + core

            @pl.when(dest != tile)
            def _():
                relay_copy(h, dest).start()

    relay_steps = 2 * zone_chips

    @pl.when(inner)
    def _():
        copies = list(block_copies())
        copies[halves].wait()
        for h in range(halves):
            copies[h].wait()
            span = pl.ds(h * part, part)
            block = jnp.concatenate([relay_block[g, span] for g in range(groups)], axis=1)

            def relay_step(j, carry):
                pack(block, relay_target, relay_chip(j), relay_buf, span)

                @pl.when(j > 0)
                def _():
                    relay_send(h, j - 1)

                if h:

                    @pl.when(j == 0)
                    def _():
                        relay_send(h - 1, relay_steps - 1)

                return carry

            lax.fori_loop(0, relay_steps, relay_step, 0)

    lax.fori_loop(n // 2, n, spread_rows, 0)

    @pl.when(inner)
    def _():
        relay_send(halves - 1, relay_steps - 1)
        relay_own.start()

    own_piece.wait()
    spread_out = pltpu.make_async_copy(spread, spread_ref, local_sem.at[2])
    spread_out.start()
    for k in range(1, nm):
        member_copy(k).wait()

    def mix(l, carry):
        total = jnp.broadcast_to(
            mean_ref[l].astype(jnp.float32), (weight_ref.shape[1], cols)
        )
        mixture = jnp.zeros_like(total)
        for p in range(nm):
            mixture = mixture + jnp.dot(
                weight_ref[p], pieces[p, l], preferred_element_type=jnp.float32
            )
        mixed[l] = (total + mixture).astype(jnp.bfloat16)
        return carry

    lax.fori_loop(0, levels, mix, 0)

    analysis_out = pltpu.make_async_copy(mixed, analysis_ref, local_sem.at[3])
    analysis_out.start()

    def drain(k, carry):
        other = lax.rem(tile + k, n)
        same_half = (other // zone_tiles) // 2 == far_half

        @pl.when(jnp.logical_or(jnp.logical_not(inner), same_half))
        def _():
            tile_copy(other).wait_send()

        @pl.when(jnp.logical_and(inner, same_half))
        def _():
            for h in range(halves):
                relay_copy(h, other).wait_send()

        @pl.when(jnp.logical_not(jnp.logical_and(inner, other == partner)))
        def _():
            arrival(other).wait_recv()

        return carry

    lax.fori_loop(1, n, drain, 0)

    @pl.when(inner)
    def _():
        relay_own.wait()

    own_chunk.wait()
    spread_out.wait()
    analysis_out.wait()


def relay_split(rows):
    return 2 if rows % 32 == 0 else 1


def combine_kernel(n, groups, per_step, bias_ref, recv_ref, spread_ref, out_ref):
    step = pl.program_id(0)
    slots = spread_ref.shape[0] // n
    per_group = out_ref.shape[1] * pl.num_programs(0)
    members = out_ref.shape[2]
    blocks = [recv_ref[s] for s in range(n)]
    for g in range(groups):
        lanes = slice(g * slots, (g + 1) * slots)
        stacked = jnp.concatenate([block[:, lanes] for block in blocks], axis=1)
        prior = jnp.dot(stacked, spread_ref[...], preferred_element_type=jnp.float32)
        for c in range(per_step):
            bias = bias_ref[g * per_group + step * per_step + c]
            out_ref[g, c] = prior[c * members : (c + 1) * members, :] + bias


def shards(
    n,
    nm,
    anomalies,
    analysis_weights,
    background_mean,
    background,
    jacobian_table,
    channel_list,
    send_slots,
    footprint,
    footprint_weight,
    channel_bias,
):
    mem_dev, levels, cols = anomalies.shape
    channels = channel_list.shape[0]
    slots = send_slots.shape[2]
    obs = footprint.shape[0]
    groups = LANES // slots
    rows = channels * mem_dev // groups
    halves = relay_split(rows)
    mem = lax.axis_index("mem")

    chosen = (
        jnp.arange(jacobian_table.shape[0], dtype=jnp.int32)[:, None] == channel_list[None, :]
    ).astype(jnp.bfloat16)
    selected = jnp.einsum(
        "sl,sc->cl", jacobian_table, chosen, preferred_element_type=jnp.float32
    ).astype(jnp.bfloat16)
    owned = jnp.einsum(
        "cl,klx->ckx", selected, background, preferred_element_type=jnp.float32
    ).astype(jnp.bfloat16)
    owned = owned.reshape(groups, rows, cols)
    lane_rows = jnp.maximum(send_slots[0], 0)[:, None, :] + (
        jnp.arange(groups, dtype=jnp.int32) * cols
    )[None, :, None]
    target = lane_rows.reshape(n, 1, LANES)
    weights = lax.dynamic_slice_in_dim(analysis_weights[0], mem * mem_dev, mem_dev, 1)
    weights = jnp.transpose(weights.reshape(nm, mem_dev, mem_dev), (0, 2, 1))
    vmem = pl.BlockSpec(memory_space=pltpu.VMEM)
    hbm = pl.BlockSpec(memory_space=pl.ANY)
    received, analysis, spread = pl.pallas_call(
        functools.partial(exchange_kernel, n, nm),
        out_shape=(
            jax.ShapeDtypeStruct((n, rows, LANES), jnp.bfloat16),
            jax.ShapeDtypeStruct((levels, mem_dev, cols), jnp.bfloat16),
            jax.ShapeDtypeStruct((n * slots, obs), jnp.bfloat16),
        ),
        in_specs=[vmem, vmem, hbm, vmem, vmem, vmem, vmem],
        out_specs=(hbm, hbm, hbm),
        scratch_shapes=[
            pltpu.VMEM((n, rows, LANES), jnp.bfloat16),
            pltpu.VMEM((n, rows, LANES), jnp.bfloat16),
            pltpu.VMEM((groups, rows, cols), jnp.bfloat16),
            pltpu.VMEM((n, 1, LANES), jnp.int32),
            pltpu.VMEM((nm, levels, mem_dev, cols), jnp.bfloat16),
            pltpu.VMEM((levels, mem_dev, cols), jnp.bfloat16),
            pltpu.VMEM((n * slots, obs), jnp.bfloat16),
            pltpu.SemaphoreType.DMA((n,)),
            pltpu.SemaphoreType.DMA((n,)),
            pltpu.SemaphoreType.DMA((nm,)),
            pltpu.SemaphoreType.DMA((nm,)),
            pltpu.SemaphoreType.DMA((halves + 1,)),
            pltpu.SemaphoreType.DMA((halves + 1,)),
            pltpu.SemaphoreType.DMA((halves, n)),
            pltpu.SemaphoreType.DMA((5,)),
        ],
        compiler_params=pltpu.CompilerParams(
            collective_id=0, has_side_effects=True, vmem_limit_bytes=48 * 1024 * 1024
        ),
        name="exchange",
    )(
        owned,
        target,
        jnp.transpose(anomalies, (1, 0, 2)),
        weights,
        background_mean[:, None, :],
        jnp.transpose(footprint),
        jnp.transpose(footprint_weight),
    )
    analysis_members = jnp.transpose(analysis, (1, 0, 2))

    per_group = channels // groups
    per_step = next(c for c in (4, 8, per_group) if c * mem_dev % 16 == 0)
    prior = pl.pallas_call(
        functools.partial(combine_kernel, n, groups, per_step),
        out_shape=jax.ShapeDtypeStruct((groups, per_group, mem_dev, obs), jnp.float32),
        grid=(per_group // per_step,),
        in_specs=[
            pl.BlockSpec(memory_space=pltpu.SMEM),
            pl.BlockSpec((n, per_step * mem_dev, LANES), lambda i: (0, i, 0)),
            pl.BlockSpec((n * slots, obs), lambda i: (0, 0)),
        ],
        out_specs=pl.BlockSpec((groups, per_step, mem_dev, obs), lambda i: (0, i, 0, 0)),
        compiler_params=pltpu.CompilerParams(vmem_limit_bytes=48 * 1024 * 1024),
        name="combine",
    )(channel_bias, received, spread)
    return analysis_members, prior.reshape(channels, mem_dev, obs)


def solution(mesh):
    placed = (
        P("mem", None, "tile"),
        P("tile", None, None),
        P(None, "tile"),
        P("mem", None, "tile"),
        P(),
        P(),
        P("tile", None, None),
        P("tile", None),
        P("tile", None),
        P(),
    )
    return jax.shard_map(
        functools.partial(shards, mesh.shape["tile"], mesh.shape["mem"]),
        mesh=mesh,
        in_specs=placed,
        out_specs=(P("mem", None, "tile"), P(None, "mem", "tile")),
        check_vma=False,
    )
```

```python
import functools

import jax
import jax.numpy as jnp
from jax import lax
from jax.experimental import pallas as pl
from jax.experimental.pallas import tpu as pltpu
from jax.sharding import PartitionSpec as P

LANES = 128
MESH = pl.DeviceIdType.MESH


def exchange_kernel(
    n,
    nm,
    owned_ref,
    target_ref,
    anom_ref,
    weight_ref,
    mean_ref,
    foot_ref,
    fweight_ref,
    recv_ref,
    analysis_ref,
    spread_ref,
    send_buf,
    relay_buf,
    relay_block,
    relay_target,
    pieces,
    mixed,
    spread,
    mean_wide,
    a_send,
    a_recv,
    m_send,
    m_recv,
    b_send,
    b_recv,
    r_send,
    local_sem,
):
    tile = lax.axis_index("tile")
    mem = lax.axis_index("mem")
    groups, rows, cols = owned_ref.shape
    chips = n // 2
    slots = spread_ref.shape[0] // n
    obs = spread_ref.shape[1]
    levels = anom_ref.shape[0]

    barrier = pltpu.get_barrier_semaphore()

    def greet(k, carry):
        pl.semaphore_signal(
            barrier, inc=1, device_id=(lax.rem(tile + k, n), mem), device_id_type=MESH
        )
        return carry

    lax.fori_loop(1, n, greet, 0)
    for k in range(1, nm):
        pl.semaphore_signal(
            barrier, inc=1, device_id=(tile, lax.rem(mem + k, nm)), device_id_type=MESH
        )
    own_piece = pltpu.make_async_copy(anom_ref, pieces.at[mem], local_sem.at[0])
    own_piece.start()
    pl.semaphore_wait(barrier, n - 1 + nm - 1)

    def member_copy(k):
        peer = lax.rem(mem + k, nm)
        return pltpu.make_async_remote_copy(
            src_ref=anom_ref,
            dst_ref=pieces.at[mem],
            send_sem=m_send.at[k],
            recv_sem=m_recv.at[k],
            device_id=(tile, peer),
            device_id_type=MESH,
        )

    for k in range(1, nm):
        member_copy(k).start()

    zone_tiles = n // 4
    zone_chips = chips // 4
    zone = tile // zone_tiles
    far_half = zone // 2
    near = zone - 3 * far_half
    depth = near * (1 - 2 * far_half)
    inner = depth == 1
    partner = lax.rem(tile + (1 - 2 * far_half) * zone_tiles + n, n)
    my_chip = tile // 2
    my_place = lax.rem(my_chip, zone_chips)
    halves = relay_split(rows)
    part = rows // halves

    def block_copies():
        for h in range(halves):
            span = (slice(None), pl.ds(h * part, part), slice(None))
            yield pltpu.make_async_remote_copy(
                src_ref=owned_ref.at[span],
                dst_ref=relay_block.at[span],
                send_sem=b_send.at[h],
                recv_sem=b_recv.at[h],
                device_id=(partner, mem),
                device_id_type=MESH,
            )
        yield pltpu.make_async_remote_copy(
            src_ref=target_ref,
            dst_ref=relay_target,
            send_sem=b_send.at[halves],
            recv_sem=b_recv.at[halves],
            device_id=(partner, mem),
            device_id_type=MESH,
        )

    @pl.when(inner)
    def _():
        for copy in reversed(list(block_copies())):
            copy.start()

    def tile_copy(dest):
        return pltpu.make_async_remote_copy(
            src_ref=send_buf.at[dest],
            dst_ref=recv_ref.at[tile],
            send_sem=a_send.at[dest],
            recv_sem=a_recv.at[tile],
            device_id=(dest, mem),
            device_id_type=MESH,
        )

    def relay_copy(h, dest):
        return pltpu.make_async_remote_copy(
            src_ref=relay_buf.at[dest, pl.ds(h * part, part)],
            dst_ref=recv_ref.at[partner, pl.ds(h * part, part)],
            send_sem=r_send.at[h, dest],
            recv_sem=a_recv.at[partner],
            device_id=(dest, mem),
            device_id_type=MESH,
        )

    def arrival(source):
        return pltpu.make_async_remote_copy(
            src_ref=send_buf.at[source],
            dst_ref=recv_ref.at[source],
            send_sem=a_send.at[source],
            recv_sem=a_recv.at[source],
            device_id=(source, mem),
            device_id_type=MESH,
        )

    def chip_of(their_zone, r):
        their_zone = their_zone + far_half * (3 - 2 * their_zone)
        return their_zone * zone_chips + lax.rem(my_place + r, zone_chips)

    def direct_chip(j):
        k = j // zone_chips
        outer_zone = k + (k // 2) * (5 - 2 * k)
        return chip_of(outer_zone + depth * (1 - k - outer_zone), lax.rem(j, zone_chips))

    row_id = lax.broadcasted_iota(jnp.int32, (groups * cols, 2 * LANES), 0)

    def pack(wide, table_ref, chip, out_ref, span):
        first = chip * 2
        want = jnp.concatenate([table_ref[first], table_ref[first + 1]], axis=1)
        pick = jnp.where(row_id == want, 1.0, 0.0).astype(jnp.bfloat16)
        out = jnp.dot(wide, pick, preferred_element_type=jnp.float32).astype(jnp.bfloat16)
        out_ref[first, span] = out[:, :LANES]
        out_ref[first + 1, span] = out[:, LANES:]

    def send(chip):
        for core in range(2):
            dest = chip * 2 + core

            @pl.when(dest != tile)
            def _():
                tile_copy(dest).start()

    wide = jnp.concatenate([owned_ref[g] for g in range(groups)], axis=1)
    whole = slice(None)
    pack(wide, target_ref, direct_chip(0), send_buf, whole)

    def step(j, carry):
        pack(wide, target_ref, direct_chip(j), send_buf, whole)
        send(direct_chip(j - 1))
        return carry

    steps = zone_chips * (4 - 2 * depth)
    lax.fori_loop(1, steps, step, 0)
    own_chunk = pltpu.make_async_copy(send_buf.at[tile], recv_ref.at[tile], local_sem.at[1])
    own_chunk.start()

    fweight = fweight_ref[...].astype(jnp.float32)

    def spread_rows(s, carry):
        ids = lax.broadcasted_iota(jnp.int32, (slots, obs), 0) + s * slots
        total = jnp.zeros((slots, obs), jnp.float32)
        for j in range(foot_ref.shape[0]):
            total = total + jnp.where(
                ids == foot_ref[j : j + 1, :], fweight[j : j + 1, :], 0.0
            )
        spread[pl.ds(pl.multiple_of(s * slots, slots), slots), :] = total.astype(jnp.bfloat16)
        return carry

    lax.fori_loop(0, n // 2, spread_rows, 0)
    send(direct_chip(steps - 1))

    def relay_chip(j):
        return chip_of(j // zone_chips, lax.rem(j, zone_chips))

    relay_own = pltpu.make_async_copy(relay_buf.at[tile], recv_ref.at[partner], local_sem.at[4])

    def relay_send(h, j):
        for core in range(2):
            dest = relay_chip(j) * 2 + core

            @pl.when(dest != tile)
            def _():
                relay_copy(h, dest).start()

    relay_steps = 2 * zone_chips

    @pl.when(inner)
    def _():
        copies = list(block_copies())
        copies[halves].wait()
        for h in range(halves):
            copies[h].wait()
            span = pl.ds(h * part, part)
            block = jnp.concatenate([relay_block[g, span] for g in range(groups)], axis=1)

            def relay_step(j, carry):
                pack(block, relay_target, relay_chip(j), relay_buf, span)

                @pl.when(j > 0)
                def _():
                    relay_send(h, j - 1)

                if h:

                    @pl.when(j == 0)
                    def _():
                        relay_send(h - 1, relay_steps - 1)

                return carry

            lax.fori_loop(0, relay_steps, relay_step, 0)

    lax.fori_loop(n // 2, n, spread_rows, 0)

    @pl.when(inner)
    def _():
        relay_send(halves - 1, relay_steps - 1)
        relay_own.start()

    own_piece.wait()
    spread_out = pltpu.make_async_copy(spread, spread_ref, local_sem.at[2])
    spread_out.start()
    for k in range(1, nm):
        member_copy(k).wait()

    mean_wide[...] = mean_ref[...].astype(jnp.float32)

    def mix(l, carry):
        total = jnp.broadcast_to(
            mean_wide[pl.ds(l, 1), :], (weight_ref.shape[1], cols)
        )
        mixture = jnp.zeros_like(total)
        for p in range(nm):
            mixture = mixture + jnp.dot(
                weight_ref[p], pieces[p, l], preferred_element_type=jnp.float32
            )
        mixed[l] = (total + mixture).astype(jnp.bfloat16)
        return carry

    lax.fori_loop(0, levels, mix, 0)

    analysis_out = pltpu.make_async_copy(mixed, analysis_ref, local_sem.at[3])
    analysis_out.start()

    def drain(k, carry):
        other = lax.rem(tile + k, n)
        same_half = (other // zone_tiles) // 2 == far_half

        @pl.when(jnp.logical_or(jnp.logical_not(inner), same_half))
        def _():
            tile_copy(other).wait_send()

        @pl.when(jnp.logical_and(inner, same_half))
        def _():
            for h in range(halves):
                relay_copy(h, other).wait_send()

        @pl.when(jnp.logical_not(jnp.logical_and(inner, other == partner)))
        def _():
            arrival(other).wait_recv()

        return carry

    lax.fori_loop(1, n, drain, 0)

    @pl.when(inner)
    def _():
        relay_own.wait()

    own_chunk.wait()
    spread_out.wait()
    analysis_out.wait()


def relay_split(rows):
    return 2 if rows % 32 == 0 else 1


def combine_kernel(n, groups, per_step, bias_ref, recv_ref, spread_ref, out_ref):
    step = pl.program_id(0)
    slots = spread_ref.shape[0] // n
    per_group = out_ref.shape[1] * pl.num_programs(0)
    members = out_ref.shape[2]
    rows = recv_ref.shape[1]
    blocks = [recv_ref[s] for s in range(n)]
    stacked = jnp.concatenate(
        [
            jnp.concatenate([block[:, g * slots : (g + 1) * slots] for block in blocks], axis=1)
            for g in range(groups)
        ],
        axis=0,
    )
    prior = jnp.dot(stacked, spread_ref[...], preferred_element_type=jnp.float32)
    for g in range(groups):
        for c in range(per_step):
            first = g * rows + c * members
            bias = bias_ref[g * per_group + step * per_step + c]
            out_ref[g, c] = prior[first : first + members, :] + bias


def shards(
    n,
    nm,
    anomalies,
    analysis_weights,
    background_mean,
    background,
    jacobian_table,
    channel_list,
    send_slots,
    footprint,
    footprint_weight,
    channel_bias,
):
    mem_dev, levels, cols = anomalies.shape
    channels = channel_list.shape[0]
    slots = send_slots.shape[2]
    obs = footprint.shape[0]
    groups = LANES // slots
    rows = channels * mem_dev // groups
    halves = relay_split(rows)
    mem = lax.axis_index("mem")

    chosen = (
        jnp.arange(jacobian_table.shape[0], dtype=jnp.int32)[:, None] == channel_list[None, :]
    ).astype(jnp.bfloat16)
    selected = jnp.einsum(
        "sl,sc->cl", jacobian_table, chosen, preferred_element_type=jnp.float32
    ).astype(jnp.bfloat16)
    owned = jnp.einsum(
        "cl,klx->ckx", selected, background, preferred_element_type=jnp.float32
    ).astype(jnp.bfloat16)
    owned = owned.reshape(groups, rows, cols)
    lane_rows = jnp.maximum(send_slots[0], 0)[:, None, :] + (
        jnp.arange(groups, dtype=jnp.int32) * cols
    )[None, :, None]
    target = lane_rows.reshape(n, 1, LANES)
    weights = lax.dynamic_slice_in_dim(analysis_weights[0], mem * mem_dev, mem_dev, 1)
    weights = jnp.transpose(weights.reshape(nm, mem_dev, mem_dev), (0, 2, 1))
    vmem = pl.BlockSpec(memory_space=pltpu.VMEM)
    hbm = pl.BlockSpec(memory_space=pl.ANY)
    received, analysis, spread = pl.pallas_call(
        functools.partial(exchange_kernel, n, nm),
        out_shape=(
            jax.ShapeDtypeStruct((n, rows, LANES), jnp.bfloat16),
            jax.ShapeDtypeStruct((levels, mem_dev, cols), jnp.bfloat16),
            jax.ShapeDtypeStruct((n * slots, obs), jnp.bfloat16),
        ),
        in_specs=[vmem, vmem, hbm, vmem, vmem, vmem, vmem],
        out_specs=(hbm, hbm, hbm),
        scratch_shapes=[
            pltpu.VMEM((n, rows, LANES), jnp.bfloat16),
            pltpu.VMEM((n, rows, LANES), jnp.bfloat16),
            pltpu.VMEM((groups, rows, cols), jnp.bfloat16),
            pltpu.VMEM((n, 1, LANES), jnp.int32),
            pltpu.VMEM((nm, levels, mem_dev, cols), jnp.bfloat16),
            pltpu.VMEM((levels, mem_dev, cols), jnp.bfloat16),
            pltpu.VMEM((n * slots, obs), jnp.bfloat16),
            pltpu.VMEM((levels, cols), jnp.float32),
            pltpu.SemaphoreType.DMA((n,)),
            pltpu.SemaphoreType.DMA((n,)),
            pltpu.SemaphoreType.DMA((nm,)),
            pltpu.SemaphoreType.DMA((nm,)),
            pltpu.SemaphoreType.DMA((halves + 1,)),
            pltpu.SemaphoreType.DMA((halves + 1,)),
            pltpu.SemaphoreType.DMA((halves, n)),
            pltpu.SemaphoreType.DMA((5,)),
        ],
        compiler_params=pltpu.CompilerParams(
            collective_id=0, has_side_effects=True, vmem_limit_bytes=24 * 1024 * 1024
        ),
        name="exchange",
    )(
        owned,
        target,
        jnp.transpose(anomalies, (1, 0, 2)),
        weights,
        background_mean,
        jnp.transpose(footprint),
        jnp.transpose(footprint_weight),
    )
    analysis_members = jnp.transpose(analysis, (1, 0, 2))

    per_group = channels // groups
    per_step = next(c for c in (4, 8, per_group) if c * mem_dev % 16 == 0)
    prior = pl.pallas_call(
        functools.partial(combine_kernel, n, groups, per_step),
        out_shape=jax.ShapeDtypeStruct((groups, per_group, mem_dev, obs), jnp.float32),
        grid=(per_group // per_step,),
        in_specs=[
            pl.BlockSpec(memory_space=pltpu.SMEM),
            pl.BlockSpec((n, per_step * mem_dev, LANES), lambda i: (0, i, 0)),
            pl.BlockSpec((n * slots, obs), lambda i: (0, 0)),
        ],
        out_specs=pl.BlockSpec((groups, per_step, mem_dev, obs), lambda i: (0, i, 0, 0)),
        compiler_params=pltpu.CompilerParams(vmem_limit_bytes=24 * 1024 * 1024),
        name="combine",
    )(channel_bias, received, spread)
    return analysis_members, prior.reshape(channels, mem_dev, obs)


def solution(mesh):
    placed = (
        P("mem", None, "tile"),
        P("tile", None, None),
        P(None, "tile"),
        P("mem", None, "tile"),
        P(),
        P(),
        P("tile", None, None),
        P("tile", None),
        P("tile", None),
        P(),
    )
    return jax.shard_map(
        functools.partial(shards, mesh.shape["tile"], mesh.shape["mem"]),
        mesh=mesh,
        in_specs=placed,
        out_specs=(P("mem", None, "tile"), P(None, "mem", "tile")),
        check_vma=False,
    )
```
